32 devices in a mesh: row: 4 (over z), col: 8 (over y, x, core).
Axes of the slice: x: 2, y: 2, z: 4, core: 2. Of those that a mesh axis runs over, the one named last changes fastest.
Arguments:
- tokens: bfloat16 [3072, 8192], P(('row', 'col')), may hold values from -6 to 6
- up_weight: bfloat16 [8192, 14336], P('row', 'col'), may hold values from -0.0625 to 0.0625
Outputs:
- projected: bfloat16 [3072, 14336], P('row', 'col')
The draws below stay inside these ranges and needn't reach their ends.
All inputs are finite; a program needn't handle non-finite values.
Results may differ from the reference program's by a relative error of at most 0.001.
Values may be sent and summed in bfloat16 or wider, within the bound.
A program may use at most 128 MiB of HBM per device.

```python
import jax
import jax.numpy as jnp

D = 8192
FF = 14336
TOKENS = 3072


def block_levels(stream_key, shape, pieces, least, high):
    gain = 1.0
    for axis_at, blocks in pieces:
        heights = jax.random.uniform(jax.random.fold_in(jax.random.fold_in(stream_key, 6), axis_at), (blocks,), jnp.float32, least / len(pieces), high / len(pieces))
        gain = gain * jnp.repeat(jnp.exp(heights), shape[axis_at] // blocks).reshape((-1,) + (1,) * (len(shape) - 1 - axis_at))
    return gain


def scatter_about(stream_key, extent, scale, bound, pieces=(), held_as=jnp.bfloat16):
    array = jax.random.normal(stream_key, extent, jnp.float32) * scale
    if len(pieces) > 0:
        array = block_levels(stream_key, extent, pieces, -0.22, 0.18) * array
    return jnp.clip(array, min=-bound, max=bound).astype(held_as)


def setup_inputs(seed: int = 0) -> dict:
    arg_keys = jax.random.split(jax.random.key(seed), 3)
    return {
        "tokens": scatter_about(arg_keys[0], (TOKENS, D), 1.0, 6.0, ((0, 32),)),
        "up_weight": scatter_about(arg_keys[1], (D, FF), D ** -0.5, 0.0625, ((0, 4), (1, 8))),
    }


def reference(tokens, up_weight):
    sums = jnp.dot(tokens.astype(jnp.float32), up_weight.astype(jnp.float32), preferred_element_type=jnp.float32)
    return sums.astype(jnp.bfloat16)
```

```python
import functools

import jax
import jax.numpy as jnp
from jax import lax
from jax.experimental import pallas as pl
from jax.experimental.pallas import tpu as pltpu
from jax.sharding import PartitionSpec as P

LINE, PLANE = 4, 8
WIDTH = 256
SPAN, OFFSET, LEAST = 250.0, 125.0, 1e-30
TS, TO, MS, MO = range(4)
MESH = pl.DeviceIdType.MESH


def gathered_weights(tokens, up_weight):
    w_column = lax.all_gather(up_weight, "row", axis=0, tiled=True)
    rows = lax.all_gather(tokens, "col", axis=0, tiled=True)
    return jnp.dot(rows, w_column, preferred_element_type=jnp.float32).astype(jnp.bfloat16)


def encode(sums):
    groups = sums.reshape(-1, 8, sums.shape[-1])
    most = jnp.maximum(jnp.max(jnp.abs(groups), axis=0), LEAST)
    code = jnp.exp2(jnp.abs(groups) * (SPAN / most)[None] - OFFSET)
    code = jnp.where(groups < 0, -code, code)
    return code.reshape(sums.shape).astype(jnp.bfloat16), most


def decode(code, most):
    groups = code.astype(jnp.float32).reshape(-1, 8, code.shape[-1])
    size = (jnp.log2(jnp.abs(groups)) + OFFSET) * (most * (1.0 / SPAN))[None]
    return jnp.where(groups < 0, -size, size).reshape(code.shape)


def kernel(
    tok, w, out, tbuf, wbuf, code_out, code_in, most_out, most_in, result,
    wl_sem, ws_sem, wr_sem, zs_sem, zr_sem, gs_sem, gr_sem, ms_sem, mr_sem, cs_sem, cr_sem, os_sem, or_sem,
):
    z, q = lax.axis_index("row"), lax.axis_index("col")
    piece, half = tok.shape[0], tok.shape[1] // 2
    depth = w.shape[0]
    chunks = wbuf.shape[0]
    rows = tbuf.shape[1]
    blocks = most_out.shape[2]
    block = rows // blocks
    mine = z // 2
    own_slot = z % 2

    def half_of(h):
        return tok.at[:, pl.ds(pl.multiple_of(h * half, half), half)]

    def place(kind, at):
        return tbuf.at[kind, pl.ds(pl.multiple_of(at * piece, piece), piece), :]

    def w_slot(j, slot):
        return wbuf.at[j, pl.ds(pl.multiple_of(slot * depth, depth), depth), :]

    def columns(ref, j):
        return ref.at[:, pl.ds(pl.multiple_of(j * WIDTH, WIDTH), WIDTH)]

    def remote(src, dst, send, recv, device):
        return pltpu.make_async_remote_copy(
            src_ref=src, dst_ref=dst, send_sem=send, recv_sem=recv, device_id=device, device_id_type=MESH
        )

    barrier = pltpu.get_barrier_semaphore()

    def greet(devices):
        for device in devices:
            pl.semaphore_signal(barrier, inc=1, device_id=device, device_id_type=MESH)
        pl.semaphore_wait(barrier, len(devices))

    @pl.when((z == 0) | (z == LINE - 1))
    def outer():
        near, beyond = 1 + mine, 2 - mine
        greet([(near, q), (beyond, q)])
        far_tokens = remote(half_of(1 - mine), place(TO, q), zs_sem.at[TO], zr_sem.at[TO], (beyond, q))
        near_tokens = remote(half_of(mine), place(MO, q), zs_sem.at[MO], zr_sem.at[MO], (near, q))
        far_tokens.start()
        near_tokens.start()

        def weight(j):
            return remote(columns(w, j), w_slot(j, own_slot), ws_sem.at[j], wr_sem.at[j], (near, q))

        @pl.loop(0, chunks)
        def _(j):
            weight(j).start()

        far_tokens.wait_send()
        near_tokens.wait_send()

        @pl.loop(0, chunks)
        def _(j):
            weight(j).wait_send()

        @pl.loop(0, chunks)
        def _(j):
            remote(result.at[1, j], columns(out, j), os_sem.at[1, j], or_sem.at[j], (near, q)).wait_recv()

    @pl.when((z != 0) & (z != LINE - 1))
    def inner():
        across = (LINE - 1 - z, q)
        end = mine * (LINE - 1)
        below, other_end = (end, q), (LINE - 1 - end, q)
        c, x, y = q % 2, (q // 2) % 2, q // 4
        over_x, over_y = q + 2 - 4 * x, q + 4 - 8 * y
        a = (1 - c) * over_x + c * over_y
        b = (1 - c) * over_y + c * over_x
        to_sib = 1 - 2 * c
        diagonal = over_x + over_y - q
        sib = q + to_sib
        greet([across, below, other_end, (z, a), (z, b), (z, sib)])

        def plane(kind, at, n, slot, device, src=None):
            here = place(kind, at)
            return remote(here if src is None else src, here, gs_sem.at[kind, n], gr_sem.at[kind, slot], (z, device))

        def own(kind, src=None):
            return [plane(kind, q, 0, 1, a, src), plane(kind, q, 1, 2, b, src), plane(kind, q, 2, 4, sib, src)]

        def from_a(kind):
            return [plane(kind, a, 3, 3, b), plane(kind, a, 4, 5, sib)]

        def from_b(kind):
            return [plane(kind, b, 5, 6, sib)]

        def from_d(kind):
            return [plane(kind, diagonal, 6, 7, sib)]

        def arrived(kind, at, slot, device):
            remote(place(kind, at), place(kind, at), gs_sem.at[kind, 0], gr_sem.at[kind, slot], (z, device)).wait_recv()

        def start(copies):
            for copy in copies:
                copy.start()

        def on_a(kind):
            arrived(kind, a, 1, a)
            start(from_a(kind))

        def on_b(kind):
            arrived(kind, b, 2, b)
            start(from_b(kind))

        def on_d(kind):
            arrived(kind, diagonal, 3, b)
            start(from_d(kind))

        def finish(kind):
            for at, slot in ((sib, 4), (b + to_sib, 5), (a + to_sib, 6), (diagonal + to_sib, 7)):
                arrived(kind, at, slot, sib)

        def z_tokens(kind, device):
            return remote(half_of(1 - mine), place(kind, q), zs_sem.at[kind], zr_sem.at[kind], device)

        def on_z(kind, device):
            z_tokens(kind, device).wait_recv()
            start(own(kind))

        own_half = half_of(mine)
        mine_here = pltpu.make_async_copy(own_half, place(MS, q), zr_sem.at[MS])

        def w_here(j):
            return pltpu.make_async_copy(columns(w, j), w_slot(j, own_slot), wl_sem.at[j])

        def w_far(j):
            return remote(columns(w, j), w_slot(j, 1 - own_slot), ws_sem.at[j], wr_sem.at[j], below)

        def sums_out(k, j):
            return [
                remote(code_out.at[k, j], code_in.at[k, j], ms_sem.at[k, j], mr_sem.at[k, j], across),
                remote(most_out.at[k, j], most_in.at[k, j], cs_sem.at[k, j], cr_sem.at[k, j], across),
            ]

        def result_up(j):
            return pltpu.make_async_copy(result.at[0, j], columns(out, j), os_sem.at[0, j])

        def result_out(j):
            return remote(result.at[1, j], columns(out, j), os_sem.at[1, j], or_sem.at[j], below)

        z_tokens(TS, across).start()
        start(own(MS, own_half))
        mine_here.start()

        @pl.loop(0, chunks)
        def _(j):
            w_here(j).start()

        on_z(TS, across)
        on_b(MS)
        on_a(TS)
        on_b(TS)
        on_z(TO, other_end)
        on_d(TS)
        finish(TS)
        on_a(TO)
        on_b(TO)
        on_a(MS)
        on_z(MO, below)
        on_d(TO)
        finish(TO)

        def product(kind, m, j):
            left = tbuf[kind, pl.ds(pl.multiple_of(m * block, block), block), :]
            return jnp.dot(left, wbuf[j], preferred_element_type=jnp.float32)

        def theirs(k, j):
            @pl.loop(0, blocks)
            def _(m):
                code, most = encode(product(TS + k, m, j))
                code_out[k, j, pl.ds(pl.multiple_of(m * block, block), block), :] = code
                most_out[k, j, m] = most

            start(sums_out(k, j))

        def finals(k, j):
            for copy in sums_out(k, j):
                copy.wait_recv()

            @pl.loop(0, blocks)
            def _(m):
                at = pl.ds(pl.multiple_of(m * block, block), block)
                total = product(MS + k, m, j) + decode(code_in[k, j, at, :], most_in[k, j, m])
                result[k, j, at, :] = total.astype(jnp.bfloat16)

        def finals_of(j):
            @pl.loop(0, 2)
            def _(n):
                k = 1 - n
                finals(k, j)

                @pl.when(k == 1)
                def _():
                    result_out(j).start()

                @pl.when(k == 0)
                def _():
                    result_up(j).start()

        @pl.loop(0, chunks + 1)
        def _(j):
            @pl.when(j < chunks)
            def _():
                w_here(j).wait()
                w_far(j).wait_recv()

                @pl.loop(0, 2)
                def _(n):
                    theirs(1 - n, j)

            @pl.when(j == 0)
            def _():
                mine_here.wait()
                on_d(MS)
                on_a(MO)
                on_b(MO)
                on_d(MO)
                finish(MS)
                finish(MO)

            @pl.when(j > 0)
            def _():
                finals_of(j - 1)

        z_tokens(TS, across).wait_send()
        for kind in range(4):
            for copy in own(kind, own_half if kind == MS else None) + from_a(kind) + from_b(kind) + from_d(kind):
                copy.wait_send()

        @pl.loop(0, chunks)
        def _(j):
            for k in range(2):
                for copy in sums_out(k, j):
                    copy.wait_send()
            result_up(j).wait()
            result_out(j).wait_send()


def line_plan(tokens, up_weight):
    piece, features = tokens.shape
    depth, columns = up_weight.shape
    rows, chunks, blocks = piece * PLANE, columns // WIDTH, 2
    dma = pltpu.SemaphoreType.DMA
    sums = (2, chunks, rows, WIDTH)
    mosts = (2, chunks, blocks, 8, WIDTH)
    return pl.pallas_call(
        kernel,
        out_shape=jax.ShapeDtypeStruct((rows, columns), jnp.bfloat16),
        in_specs=[pl.BlockSpec(memory_space=pl.ANY)] * 2,
        out_specs=pl.BlockSpec(memory_space=pl.ANY),
        scratch_shapes=[
            pltpu.VMEM((4, rows, features // 2), jnp.bfloat16),
            pltpu.VMEM((chunks, 2 * depth, WIDTH), jnp.bfloat16),
            pltpu.VMEM(sums, jnp.bfloat16),
            pltpu.VMEM(sums, jnp.bfloat16),
            pltpu.VMEM(mosts, jnp.float32),
            pltpu.VMEM(mosts, jnp.float32),
            pltpu.VMEM(sums, jnp.bfloat16),
            dma((chunks,)), dma((chunks,)), dma((chunks,)),
            dma((4,)), dma((4,)),
            dma((4, 7)), dma((4, 8)),
            dma((2, chunks)), dma((2, chunks)),
            dma((2, chunks)), dma((2, chunks)),
            dma((2, chunks)), dma((chunks,)),
        ],
        compiler_params=pltpu.CompilerParams(
            collective_id=0, has_side_effects=True, vmem_limit_bytes=67043328
        ),
        cost_estimate=pl.CostEstimate(
            flops=2 * rows * features * columns, bytes_accessed=2 * rows * features, transcendentals=0
        ),
    )(tokens, up_weight)


def solution(mesh):
    def on_device(tokens, up_weight):
        piece, features = tokens.shape
        depth, columns = up_weight.shape
        fits = mesh.shape["row"] == LINE and mesh.shape["col"] == PLANE
        fits = fits and columns % WIDTH == 0 and piece % 16 == 0 and depth % 256 == 0 and features == LINE * depth
        return (line_plan if fits else gathered_weights)(tokens, up_weight)

    return jax.shard_map(
        on_device,
        mesh=mesh,
        in_specs=(P(("row", "col"), None), P("row", "col")),
        out_specs=P("row", "col"),
        check_vma=False,
    )
```

```python
import functools

import jax
import jax.numpy as jnp
from jax import lax
from jax.experimental import pallas as pl
from jax.experimental.pallas import tpu as pltpu
from jax.sharding import PartitionSpec as P

LINE, PLANE = 4, 8
WIDTH, NARROW, FINE = 256, 128, 2
SPAN, OFFSET, LEAST = 250.0, 125.0, 1e-30
TS, TO, MS, MO = range(4)
MESH = pl.DeviceIdType.MESH


def gathered_weights(tokens, up_weight):
    w_column = lax.all_gather(up_weight, "row", axis=0, tiled=True)
    rows = lax.all_gather(tokens, "col", axis=0, tiled=True)
    return jnp.dot(rows, w_column, preferred_element_type=jnp.float32).astype(jnp.bfloat16)


def encode(sums):
    groups = sums.reshape(-1, 8, sums.shape[-1])
    most = jnp.maximum(jnp.max(jnp.abs(groups), axis=0), LEAST)
    code = jnp.exp2(jnp.abs(groups) * (SPAN / most)[None] - OFFSET)
    code = jnp.where(groups < 0, -code, code)
    return code.reshape(sums.shape).astype(jnp.bfloat16), most


def decode(code, most):
    groups = code.astype(jnp.float32).reshape(-1, 8, code.shape[-1])
    size = (jnp.log2(jnp.abs(groups)) + OFFSET) * (most * (1.0 / SPAN))[None]
    return jnp.where(groups < 0, -size, size).reshape(code.shape)


def kernel(
    tok, w, out, tbuf, mbuf, wbuf, code_out, code_in, most_out, most_in, result, acc,
    wl_sem, ws_sem, wr_sem, zs_sem, zr_sem, gs_sem, gr_sem, ms_sem, mr_sem, cs_sem, cr_sem, os_sem,
):
    z, q = lax.axis_index("row"), lax.axis_index("col")
    piece, half = tok.shape[0], tok.shape[1] // 2
    depth = w.shape[0]
    chunks = wbuf.shape[0]
    rows = tbuf.shape[1]
    blocks = most_out.shape[2]
    block = rows // blocks
    per = WIDTH // NARROW
    wide, narrow = chunks - FINE, FINE * per
    units = wide + narrow
    mine = z // 2
    own_slot = z % 2
    c, x, y = q % 2, (q // 2) % 2, q // 4
    over_x, over_y = q + 2 - 4 * x, q + 4 - 8 * y
    a = (1 - c) * over_x + c * over_y
    b = (1 - c) * over_y + c * over_x
    to_sib = 1 - 2 * c
    diagonal = over_x + over_y - q
    sib = q + to_sib
    barrier = pltpu.get_barrier_semaphore()

    def half_of(h):
        return tok.at[:, pl.ds(pl.multiple_of(h * half, half), half)]

    def block_of(k):
        return tok.at[:, pl.ds(pl.multiple_of(k * depth, depth), depth)]

    def place(kind, at):
        at = pl.ds(pl.multiple_of(at * piece, piece), piece)
        return mbuf.at[at, :] if kind == MO else tbuf.at[kind, at, :]

    def part(unit):
        if isinstance(unit, tuple):
            t = jnp.int32(unit[0])
            return wide + t, wide + lax.div(t, per), pl.ds(pl.multiple_of(lax.rem(t, per) * NARROW, NARROW), NARROW)
        return unit, unit, pl.ds(0, WIDTH)

    def columns(ref, unit):
        if isinstance(unit, tuple):
            t = jnp.int32(unit[0])
            return ref.at[:, pl.ds(pl.multiple_of(wide * WIDTH + t * NARROW, NARROW), NARROW)]
        return ref.at[:, pl.ds(pl.multiple_of(unit * WIDTH, WIDTH), WIDTH)]

    def each_unit(body):
        pl.loop(0, wide)(body)
        pl.loop(0, narrow)(lambda t: body((t,)))

    def remote(src, dst, send, recv, device):
        return pltpu.make_async_remote_copy(
            src_ref=src, dst_ref=dst, send_sem=send, recv_sem=recv, device_id=device, device_id_type=MESH
        )

    def start(copies):
        for copy in copies:
            copy.start()

    def greet(devices):
        for device in devices:
            pl.semaphore_signal(barrier, inc=1, device_id=device, device_id_type=MESH)
        pl.semaphore_wait(barrier, len(devices))

    def plane(kind, at, n, slot, device, src=None):
        here = place(kind, at)
        return remote(here if src is None else src, here, gs_sem.at[kind, n], gr_sem.at[kind, slot], (z, device))

    def own(kind, src=None):
        return [plane(kind, q, 0, 1, a, src), plane(kind, q, 1, 2, b, src), plane(kind, q, 2, 4, sib, src)]

    def from_a(kind):
        return [plane(kind, a, 3, 3, b), plane(kind, a, 4, 5, sib)]

    def from_b(kind):
        return [plane(kind, b, 5, 6, sib)]

    def from_d(kind):
        return [plane(kind, diagonal, 6, 7, sib)]

    def sent(kind, src=None):
        for copy in own(kind, src) + from_a(kind) + from_b(kind) + from_d(kind):
            copy.wait_send()

    def arrived(kind, at, slot, device):
        remote(place(kind, at), place(kind, at), gs_sem.at[kind, 0], gr_sem.at[kind, slot], (z, device)).wait_recv()

    def on_a(kind):
        arrived(kind, a, 1, a)
        start(from_a(kind))

    def on_b(kind):
        arrived(kind, b, 2, b)
        start(from_b(kind))

    def on_d(kind):
        arrived(kind, diagonal, 3, b)
        start(from_d(kind))

    def finish(kind):
        for at, slot in ((sib, 4), (b + to_sib, 5), (a + to_sib, 6), (diagonal + to_sib, 7)):
            arrived(kind, at, slot, sib)

    def w_slot(unit, slot):
        _, j, lanes = part(unit)
        return wbuf.at[j, pl.ds(pl.multiple_of(slot * depth, depth), depth), lanes]

    def w_here(j):
        at = pl.ds(pl.multiple_of(own_slot * depth, depth), depth)
        return pltpu.make_async_copy(columns(w, j), wbuf.at[j, at, :], wl_sem.at[j])

    def rows_of(m):
        return pl.ds(m * block if isinstance(m, int) else pl.multiple_of(m * block, block), block)

    def sums(k, to, unit, m, device):
        u, j, lanes = part(unit)
        at = rows_of(m)
        return [
            remote(code_out.at[k, j, at, lanes], code_in.at[to, j, at, lanes], ms_sem.at[k, u, m], mr_sem.at[to, u, m], device),
            remote(most_out.at[k, j, m, :, lanes], most_in.at[to, j, m, :, lanes], cs_sem.at[k, u, m], cr_sem.at[to, u, m], device),
        ]

    def product(kind, m, unit, slot=None):
        _, j, lanes = part(unit)
        if kind == MO:
            left, slot = mbuf[rows_of(m), :], own_slot
        elif slot is None:
            left = tbuf[kind, rows_of(m), :]
        else:
            left = tbuf[kind, rows_of(m), pl.ds(pl.multiple_of(slot * depth, depth), depth)]
        deep = slice(None) if slot is None else pl.ds(pl.multiple_of(slot * depth, depth), depth)
        return jnp.dot(left, wbuf[j, deep, lanes], preferred_element_type=jnp.float32)

    def ahead(kind, unit):
        @pl.loop(0, blocks)
        def _(m):
            acc[kind, rows_of(m), :] = product(kind, m, unit, own_slot)

    def give(kind, k, to, unit, device):
        _, j, lanes = part(unit)

        @pl.loop(0, blocks)
        def _(m):
            if kind != MO and isinstance(unit, tuple):
                total = acc[kind, rows_of(m), :] + product(kind, m, unit, 1 - own_slot)
            else:
                total = product(kind, m, unit)
            code, most = encode(total)
            code_out[k, j, rows_of(m), lanes] = code
            most_out[k, j, m, :, lanes] = most
            start(sums(k, to, unit, m, device))

    def result_up(unit):
        u, j, lanes = part(unit)
        return pltpu.make_async_copy(result.at[j, :, lanes], columns(out, unit), os_sem.at[u])

    def conclude(kind, senders, unit):
        _, j, lanes = part(unit)
        last = isinstance(unit, tuple)
        if last:
            @pl.loop(0, blocks)
            def _(m):
                acc[2, rows_of(m), :] = product(kind, m, unit)

        @pl.loop(0, blocks)
        def _(m):
            for to, device in enumerate(senders):
                for copy in sums(0, to, unit, m, device):
                    copy.wait_recv()
            total = acc[2, rows_of(m), :] if last else product(kind, m, unit)
            for to in range(len(senders)):
                total += decode(code_in[to, j, rows_of(m), lanes], most_in[to, j, m, :, lanes])
            result[j, rows_of(m), lanes] = total.astype(jnp.bfloat16)

        result_up(unit).start()

    @pl.when((z == 0) | (z == LINE - 1))
    def outer():
        near, beyond = (1 + mine, q), (2 - mine, q)
        greet([near, beyond, (z, a), (z, b), (z, sib)])
        far_tokens = remote(half_of(1 - mine), place(TO, q), zs_sem.at[TO], zr_sem.at[TO], beyond)
        near_tokens = remote(block_of(1 + mine), place(MO, q), zs_sem.at[MO], zr_sem.at[MO], near)

        def weight(unit):
            return remote(columns(w, unit), w_slot(unit, own_slot), ws_sem.at[part(unit)[0]], wr_sem.at[part(unit)[0]], near)

        near_tokens.start()
        weight(0).start()
        far_tokens.start()
        pl.loop(1, wide)(lambda j: weight(j).start())
        pl.loop(0, narrow)(lambda t: weight((t,)).start())
        start(own(MO, block_of(z)))
        mine_here = pltpu.make_async_copy(block_of(z), place(MO, q), zr_sem.at[MO])
        mine_here.start()
        pl.loop(0, chunks)(lambda j: w_here(j).start())
        on_a(MO)
        on_b(MO)
        on_d(MO)
        mine_here.wait()
        finish(MO)
        pl.loop(0, chunks)(lambda j: w_here(j).wait())
        pl.loop(0, wide)(lambda j: conclude(MO, [near, beyond], j))
        far_tokens.wait_send()
        near_tokens.wait_send()
        sent(MO, block_of(z))

        @pl.loop(0, wide)
        def _(j):
            weight(j).wait_send()
            result_up(j).wait()

        @pl.loop(0, narrow)
        def _(t):
            weight((t,)).wait_send()
            conclude(MO, [near, beyond], (t,))

        pl.loop(0, narrow)(lambda t: result_up((t,)).wait())

    @pl.when((z != 0) & (z != LINE - 1))
    def inner():
        end = mine * (LINE - 1)
        across, below, other_end = (LINE - 1 - z, q), (end, q), (LINE - 1 - end, q)
        greet([across, below, other_end, (z, a), (z, b), (z, sib)])
        own_half = half_of(mine)
        mine_here = pltpu.make_async_copy(own_half, place(MS, q), zr_sem.at[MS])

        def z_tokens(kind, device):
            src = block_of(z) if kind == MO else half_of(1 - mine)
            return remote(src, place(kind, q), zs_sem.at[kind], zr_sem.at[kind], device)

        def on_z(kind, device):
            z_tokens(kind, device).wait_recv()
            start(own(kind))

        def w_far(unit):
            u = part(unit)[0]
            return remote(columns(w, unit), w_slot(unit, 1 - own_slot), ws_sem.at[u], wr_sem.at[u], below)

        def to_across(unit):
            give(TS, 0, 0, unit, across)

        def to_other_end(unit):
            give(TO, 1, 1, unit, other_end)

        def to_below(unit):
            give(MO, 2, 0, unit, below)

        def finals(unit):
            conclude(MS, [across], unit)

        z_tokens(TS, across).start()
        mine_here.start()
        pl.loop(0, chunks)(lambda j: w_here(j).start())
        on_z(MO, below)
        on_z(TS, across)
        on_b(MO)
        on_a(TS)
        on_b(TS)
        on_d(TS)
        on_a(MO)
        finish(TS)
        pl.loop(0, chunks)(lambda j: w_here(j).wait())
        w_far(0).wait_recv()
        to_across(0)
        on_d(MO)
        on_z(TO, other_end)
        finish(MO)
        pl.loop(0, wide)(to_below)
        on_a(TO)
        on_b(TO)
        w_far(1).wait_recv()
        to_across(1)
        on_d(TO)
        start(own(MS, own_half))
        finish(TO)
        pl.loop(0, 2)(to_other_end)
        pl.loop(0, narrow)(lambda t: to_below((t,)))
        w_far(2).wait_recv()
        to_other_end(2)
        to_across(2)
        mine_here.wait()
        on_a(MS)
        on_b(MS)
        on_d(MS)
        finish(MS)
        pl.loop(0, 2)(finals)

        @pl.loop(3, wide)
        def _(j):
            w_far(j).wait_recv()
            to_other_end(j)
            to_across(j)
            finals(j - 1)

        def done(unit):
            for k, to, device in ((0, 0, across), (1, 1, other_end), (2, 0, below)):
                for m in range(blocks):
                    for copy in sums(k, to, unit, m, device):
                        copy.wait_send()

        @pl.loop(0, narrow)
        def _(t):
            ahead(TO, (t,))
            ahead(TS, (t,))
            w_far((t,)).wait_recv()
            to_other_end((t,))
            to_across((t,))

            @pl.when(t == 1)
            def _():
                finals(wide - 1)

            @pl.when(t > 1)
            def _():
                finals((t - 2,))

        z_tokens(TS, across).wait_send()
        for kind in range(4):
            sent(kind, own_half if kind == MS else None)

        @pl.loop(0, wide)
        def _(j):
            done(j)
            result_up(j).wait()

        pl.loop(narrow - 2, narrow)(lambda t: finals((t,)))

        @pl.loop(0, narrow)
        def _(t):
            done((t,))
            result_up((t,)).wait()


def line_plan(tokens, up_weight):
    piece, features = tokens.shape
    depth, columns = up_weight.shape
    rows, chunks, blocks = piece * PLANE, columns // WIDTH, 2
    units = chunks - FINE + FINE * WIDTH // NARROW
    dma, vmem, half = pltpu.SemaphoreType.DMA, pltpu.VMEM, jnp.bfloat16
    return pl.pallas_call(
        kernel,
        out_shape=jax.ShapeDtypeStruct((rows, columns), jnp.bfloat16),
        in_specs=[pl.BlockSpec(memory_space=pl.ANY)] * 2,
        out_specs=pl.BlockSpec(memory_space=pl.ANY),
        scratch_shapes=[
            vmem((3, rows, features // 2), half),
            vmem((rows, depth), half),
            vmem((chunks, 2 * depth, WIDTH), half),
            vmem((3, chunks, rows, WIDTH), half),
            vmem((2, chunks, rows, WIDTH), half),
            vmem((3, chunks, blocks, 8, WIDTH), jnp.float32),
            vmem((2, chunks, blocks, 8, WIDTH), jnp.float32),
            vmem((chunks, rows, WIDTH), half),
            vmem((3, rows, NARROW), jnp.float32),
            dma((chunks,)), dma((units,)), dma((units,)),
            dma((4,)), dma((4,)),
            dma((4, 7)), dma((4, 8)),
            dma((3, units, blocks)), dma((2, units, blocks)),
            dma((3, units, blocks)), dma((2, units, blocks)),
            dma((units,)),
        ],
        compiler_params=pltpu.CompilerParams(
            collective_id=0, has_side_effects=True, vmem_limit_bytes=67043328
        ),
        cost_estimate=pl.CostEstimate(
            flops=2 * rows * features * columns, bytes_accessed=2 * rows * features, transcendentals=0
        ),
    )(tokens, up_weight)


def solution(mesh):
    def on_device(tokens, up_weight):
        piece, features = tokens.shape
        depth, columns = up_weight.shape
        fits = columns >= (3 + FINE) * WIDTH and mesh.shape["row"] == LINE and mesh.shape["col"] == PLANE
        fits = fits and columns % WIDTH == 0 and piece % 16 == 0 and depth % 256 == 0 and features == LINE * depth
        return (line_plan if fits else gathered_weights)(tokens, up_weight)

    return jax.shard_map(
        on_device,
        mesh=mesh,
        in_specs=(P(("row", "col"), None), P("row", "col")),
        out_specs=P("row", "col"),
        check_vma=False,
    )
```

```python
import functools

import jax
import jax.numpy as jnp
from jax import lax
from jax.experimental import pallas as pl
from jax.experimental.pallas import tpu as pltpu
from jax.sharding import PartitionSpec as P

LINE, PLANE = 4, 8
WIDTH, NARROW, FINE = 256, 128, 2
SPAN, OFFSET, LEAST, GROUP = 250.0, 125.0, 1e-30, 16
TS, TO, MS, MO = range(4)
MESH = pl.DeviceIdType.MESH


def gathered_weights(tokens, up_weight):
    w_column = lax.all_gather(up_weight, "row", axis=0, tiled=True)
    rows = lax.all_gather(tokens, "col", axis=0, tiled=True)
    return jnp.dot(rows, w_column, preferred_element_type=jnp.float32).astype(jnp.bfloat16)


def encode(sums):
    groups = sums.reshape(-1, GROUP, sums.shape[-1])
    most = jnp.maximum(jnp.max(jnp.abs(groups), axis=0), LEAST).astype(jnp.bfloat16)
    code = jnp.exp2(jnp.abs(groups) * (SPAN / most.astype(jnp.float32))[None] - OFFSET)
    code = jnp.where(groups < 0, -code, code)
    return code.reshape(sums.shape).astype(jnp.bfloat16), most


def decode(code, most):
    groups = code.astype(jnp.float32).reshape(-1, GROUP, code.shape[-1])
    size = (jnp.log2(jnp.abs(groups)) + OFFSET) * (most.astype(jnp.float32) * (1.0 / SPAN))[None]
    return jnp.where(groups < 0, -size, size).reshape(code.shape)


def kernel(
    tok, w, out, tbuf, mbuf, wbuf, code_out, code_in, acc,
    wl_sem, ws_sem, wr_sem, zs_sem, zr_sem, gs_sem, gr_sem, ms_sem, mr_sem,
):
    z, q = lax.axis_index("row"), lax.axis_index("col")
    piece, half = tok.shape[0], tok.shape[1] // 2
    depth = w.shape[0]
    chunks = wbuf.shape[0]
    rows = tbuf.shape[1]
    blocks = code_out.shape[2]
    block = rows // blocks
    per = WIDTH // NARROW
    wide, narrow = chunks - FINE, FINE * per
    units = wide + narrow
    mine = z // 2
    own_slot = z % 2
    c, x, y = q % 2, (q // 2) % 2, q // 4
    over_x, over_y = q + 2 - 4 * x, q + 4 - 8 * y
    a = (1 - c) * over_x + c * over_y
    b = (1 - c) * over_y + c * over_x
    to_sib = 1 - 2 * c
    diagonal = over_x + over_y - q
    sib = q + to_sib
    barrier = pltpu.get_barrier_semaphore()

    def half_of(h):
        return tok.at[:, pl.ds(pl.multiple_of(h * half, half), half)]

    def block_of(k):
        return tok.at[:, pl.ds(pl.multiple_of(k * depth, depth), depth)]

    def place(kind, at):
        at = pl.ds(pl.multiple_of(at * piece, piece), piece)
        return mbuf.at[at, :] if kind == MO else tbuf.at[kind, at, :]

    def part(unit):
        if isinstance(unit, tuple):
            t = jnp.int32(unit[0])
            return wide + t, wide + lax.div(t, per), pl.ds(pl.multiple_of(lax.rem(t, per) * NARROW, NARROW), NARROW)
        return unit, unit, pl.ds(0, WIDTH)

    def columns(ref, unit):
        if isinstance(unit, tuple):
            t = jnp.int32(unit[0])
            return ref.at[:, pl.ds(pl.multiple_of(wide * WIDTH + t * NARROW, NARROW), NARROW)]
        return ref.at[:, pl.ds(pl.multiple_of(unit * WIDTH, WIDTH), WIDTH)]

    def each_unit(body):
        pl.loop(0, wide)(body)
        pl.loop(0, narrow)(lambda t: body((t,)))

    def remote(src, dst, send, recv, device):
        return pltpu.make_async_remote_copy(
            src_ref=src, dst_ref=dst, send_sem=send, recv_sem=recv, device_id=device, device_id_type=MESH
        )

    def start(copies):
        for copy in copies:
            copy.start()

    def greet(devices):
        for device in devices:
            pl.semaphore_signal(barrier, inc=1, device_id=device, device_id_type=MESH)
        pl.semaphore_wait(barrier, len(devices))

    def plane(kind, at, slot, device, src=None):
        here = place(kind, at)
        return remote(here if src is None else src, here, gs_sem.at[kind], gr_sem.at[kind, slot], (z, device))

    def own(kind, src=None):
        return [plane(kind, q, 0, a, src), plane(kind, q, 1, b, src), plane(kind, q, 3, sib, src)]

    def from_a(kind):
        return [plane(kind, a, 2, b), plane(kind, a, 3, sib)]

    def from_b(kind):
        return [plane(kind, b, 3, sib)]

    def from_d(kind):
        return [plane(kind, diagonal, 3, sib)]

    def pieces(kind, n):
        at = pl.ds(0, n * piece)
        return mbuf.at[at, :] if kind == MO else tbuf.at[kind, at, :]

    def sent(kind):
        remote(pieces(kind, 7), pieces(kind, 7), gs_sem.at[kind], gr_sem.at[kind, 0], (z, sib)).wait_send()

    def arrived(kind, n, slot, device):
        remote(pieces(kind, n), pieces(kind, n), gs_sem.at[kind], gr_sem.at[kind, slot], (z, device)).wait_recv()

    def on_a(kind):
        arrived(kind, 1, 0, a)
        start(from_a(kind))

    def on_b(kind):
        arrived(kind, 1, 1, b)
        start(from_b(kind))

    def on_d(kind):
        arrived(kind, 1, 2, b)
        start(from_d(kind))

    def finish(kind):
        arrived(kind, 4, 3, sib)

    def w_slot(unit, slot):
        _, j, lanes = part(unit)
        return wbuf.at[j, pl.ds(pl.multiple_of(slot * depth, depth), depth), lanes]

    def w_here(j):
        at = pl.ds(pl.multiple_of(own_slot * depth, depth), depth)
        return pltpu.make_async_copy(columns(w, j), wbuf.at[j, at, :], wl_sem.at[0])

    def rows_of(m):
        return pl.ds(m * block if isinstance(m, int) else pl.multiple_of(m * block, block), block)

    def sums(k, to, unit, m, device):
        u, j, lanes = part(unit)
        return remote(
            code_out.at[k, j, m, :, lanes], code_in.at[to, j, m, :, lanes], ms_sem.at[k], mr_sem.at[to, u, m], device
        )

    def product(kind, m, unit, slot=None):
        _, j, lanes = part(unit)
        if kind == MO:
            left, slot = mbuf[rows_of(m), :], own_slot
        elif slot is None:
            left = tbuf[kind, rows_of(m), :]
        else:
            left = tbuf[kind, rows_of(m), pl.ds(pl.multiple_of(slot * depth, depth), depth)]
        deep = slice(None) if slot is None else pl.ds(pl.multiple_of(slot * depth, depth), depth)
        return jnp.dot(left, wbuf[j, deep, lanes], preferred_element_type=jnp.float32)

    def ahead(kind, n):
        @pl.loop(0, blocks)
        def _(m):
            acc[kind, n, rows_of(m), :] = product(kind, m, wide + n, own_slot)

    def rest_of(kind, m, unit):
        _, j, lanes = part(unit)
        return acc[kind, j - wide, rows_of(m), lanes] + product(kind, m, unit, 1 - own_slot)

    def give(kind, k, to, unit, device):
        _, j, lanes = part(unit)

        @pl.loop(0, blocks)
        def _(m):
            if kind != MO and isinstance(unit, tuple):
                total = rest_of(kind, m, unit)
            else:
                total = product(kind, m, unit)
            code, most = encode(total)
            code_out[k, j, m, pl.ds(0, block), lanes] = code
            code_out[k, j, m, pl.ds(block, GROUP), lanes] = most
            sums(k, to, unit, m, device).start()

    def conclude(kind, senders, unit):
        _, j, lanes = part(unit)
        last = isinstance(unit, tuple)
        if last:
            @pl.loop(0, blocks)
            def _(m):
                acc[MS, j - wide, rows_of(m), lanes] = rest_of(kind, m, unit) if kind == MS else product(kind, m, unit)

        @pl.loop(0, blocks)
        def _(m):
            for to, device in enumerate(senders):
                sums(0, to, unit, m, device).wait_recv()
            total = acc[MS, j - wide, rows_of(m), lanes] if last else product(kind, m, unit)
            for to in range(len(senders)):
                total += decode(code_in[to, j, m, pl.ds(0, block), lanes], code_in[to, j, m, pl.ds(block, GROUP), lanes])
            at = wide * WIDTH + unit[0] * NARROW if last else unit * WIDTH
            wide_at = pl.ds(pl.multiple_of(jnp.int32(at), NARROW), NARROW if last else WIDTH)
            out[rows_of(m), wide_at] = total.astype(jnp.bfloat16)

    @pl.when((z == 0) | (z == LINE - 1))
    def outer():
        near, beyond = (1 + mine, q), (2 - mine, q)
        greet([near, beyond, (z, a), (z, b), (z, sib)])
        far_tokens = remote(half_of(1 - mine), place(TO, q), zs_sem.at[TO], zr_sem.at[TO], beyond)
        near_tokens = remote(block_of(1 + mine), place(MO, q), zs_sem.at[MO], zr_sem.at[MO], near)

        def weight(unit):
            return remote(columns(w, unit), w_slot(unit, own_slot), ws_sem.at[0], wr_sem.at[part(unit)[0]], near)

        near_tokens.start()
        weight(0).start()
        far_tokens.start()
        pl.loop(1, wide)(lambda j: weight(j).start())
        pl.loop(0, narrow)(lambda t: weight((t,)).start())
        start(own(MO, block_of(z)))
        mine_here = pltpu.make_async_copy(block_of(z), place(MO, q), zr_sem.at[MO])
        mine_here.start()
        pl.loop(0, chunks)(lambda j: w_here(j).start())
        on_a(MO)
        on_b(MO)
        on_d(MO)
        mine_here.wait()
        finish(MO)
        pltpu.make_async_copy(w, w, wl_sem.at[0]).wait()
        pl.loop(0, wide)(lambda j: conclude(MO, [near, beyond], j))
        far_tokens.wait_send()
        near_tokens.wait_send()
        sent(MO)
        remote(w, w, ws_sem.at[0], wr_sem.at[0], near).wait_send()
        pl.loop(0, narrow)(lambda t: conclude(MO, [near, beyond], (t,)))

    @pl.when((z != 0) & (z != LINE - 1))
    def inner():
        end = mine * (LINE - 1)
        across, below, other_end = (LINE - 1 - z, q), (end, q), (LINE - 1 - end, q)
        greet([across, below, other_end, (z, a), (z, b), (z, sib)])
        own_half = half_of(mine)
        mine_here = pltpu.make_async_copy(own_half, place(MS, q), zr_sem.at[MS])

        def z_tokens(kind, device):
            src = block_of(z) if kind == MO else half_of(1 - mine)
            return remote(src, place(kind, q), zs_sem.at[kind], zr_sem.at[kind], device)

        def on_z(kind, device):
            z_tokens(kind, device).wait_recv()
            start(own(kind))

        def w_far(unit):
            u = part(unit)[0]
            return remote(columns(w, unit), w_slot(unit, 1 - own_slot), ws_sem.at[0], wr_sem.at[u], below)

        def to_across(unit):
            give(TS, 0, 0, unit, across)

        def to_other_end(unit):
            give(TO, 1, 1, unit, other_end)

        def to_below(unit):
            give(MO, 2, 0, unit, below)

        def finals(unit):
            conclude(MS, [across], unit)

        z_tokens(TS, across).start()
        mine_here.start()
        pl.loop(0, chunks)(lambda j: w_here(j).start())
        on_z(MO, below)
        on_z(TS, across)
        on_b(MO)
        on_a(TS)
        on_b(TS)
        on_d(TS)
        on_a(MO)
        finish(TS)
        pltpu.make_async_copy(w, w, wl_sem.at[0]).wait()
        w_far(0).wait_recv()
        to_across(0)
        on_d(MO)
        on_z(TO, other_end)
        finish(MO)
        pl.loop(0, wide)(to_below)
        on_a(TO)
        on_b(TO)
        w_far(1).wait_recv()
        to_across(1)
        on_d(TO)
        start(own(MS, own_half))
        finish(TO)
        pl.loop(0, 2)(to_other_end)
        pl.loop(0, narrow)(lambda t: to_below((t,)))
        w_far(2).wait_recv()
        to_other_end(2)
        to_across(2)
        mine_here.wait()
        on_a(MS)
        on_b(MS)
        on_d(MS)
        finish(MS)
        pl.loop(0, 2)(finals)

        @pl.loop(3, wide)
        def _(j):
            w_far(j).wait_recv()
            to_other_end(j)
            to_across(j)
            finals(j - 1)

            @pl.when(j == 3)
            def _():
                for kind in (TO, TS, MS):
                    pl.loop(0, FINE)(lambda n: ahead(kind, n))

        @pl.loop(0, narrow)
        def _(t):
            w_far((t,)).wait_recv()
            to_other_end((t,))
            to_across((t,))

            @pl.when(t == 1)
            def _():
                finals(wide - 1)

            @pl.when(t > 1)
            def _():
                finals((t - 2,))

        z_tokens(TS, across).wait_send()
        for kind in range(4):
            sent(kind)
        pl.loop(narrow - 2, narrow)(lambda t: finals((t,)))
        for k, device in enumerate((across, other_end, below)):
            remote(code_out.at[k], code_out.at[k], ms_sem.at[k], mr_sem.at[0, 0, 0], device).wait_send()


def line_plan(tokens, up_weight):
    piece, features = tokens.shape
    depth, columns = up_weight.shape
    rows, chunks, blocks = piece * PLANE, columns // WIDTH, 2
    units = chunks - FINE + FINE * WIDTH // NARROW
    dma, vmem, half = pltpu.SemaphoreType.DMA, pltpu.VMEM, jnp.bfloat16
    return pl.pallas_call(
        kernel,
        out_shape=pltpu.VMEM((rows, columns), jnp.bfloat16),
        in_specs=[pl.BlockSpec(memory_space=pl.ANY)] * 2,
        out_specs=pl.BlockSpec(memory_space=pltpu.VMEM),
        scratch_shapes=[
            vmem((3, rows, features // 2), half),
            vmem((rows, depth), half),
            vmem((chunks, 2 * depth, WIDTH), half),
            vmem((3, chunks, blocks, rows // blocks + GROUP, WIDTH), half),
            vmem((2, chunks, blocks, rows // blocks + GROUP, WIDTH), half),
            vmem((3, FINE, rows, WIDTH), jnp.float32),
            dma((1,)), dma((1,)), dma((units,)),
            dma((4,)), dma((4,)),
            dma((4,)), dma((4, 4)),
            dma((3,)), dma((2, units, blocks)),
        ],
        compiler_params=pltpu.CompilerParams(
            collective_id=0, has_side_effects=True, vmem_limit_bytes=62914560
        ),
        cost_estimate=pl.CostEstimate(
            flops=2 * rows * features * columns, bytes_accessed=2 * rows * features, transcendentals=0
        ),
    )(tokens, up_weight)


def solution(mesh):
    def on_device(tokens, up_weight):
        piece, features = tokens.shape
        depth, columns = up_weight.shape
        fits = columns >= (4 + FINE) * WIDTH and mesh.shape["row"] == LINE and mesh.shape["col"] == PLANE
        fits = fits and columns % WIDTH == 0 and piece % 16 == 0 and depth % 256 == 0 and features == LINE * depth
        return (line_plan if fits else gathered_weights)(tokens, up_weight)

    return jax.shard_map(
        on_device,
        mesh=mesh,
        in_specs=(P(("row", "col"), None), P("row", "col")),
        out_specs=P("row", "col"),
        check_vma=False,
    )
```

```python
import functools

import jax
import jax.numpy as jnp
from jax import lax
from jax.experimental import pallas as pl
from jax.experimental.pallas import tpu as pltpu
from jax.sharding import PartitionSpec as P

LINE, PLANE = 4, 8
WIDTH, NARROW, FINE = 256, 128, 2
SPAN, OFFSET, LEAST, GROUP = 250.0, 125.0, 1e-30, 16
TS, TO, MS, MO = range(4)
MESH = pl.DeviceIdType.MESH


def gathered_weights(tokens, up_weight):
    w_column = lax.all_gather(up_weight, "row", axis=0, tiled=True)
    rows = lax.all_gather(tokens, "col", axis=0, tiled=True)
    return jnp.dot(rows, w_column, preferred_element_type=jnp.float32).astype(jnp.bfloat16)


def encode(sums):
    groups = sums.reshape(-1, GROUP, sums.shape[-1])
    most = jnp.maximum(jnp.max(jnp.abs(groups), axis=0), LEAST).astype(jnp.bfloat16)
    code = jnp.exp2(jnp.abs(groups) * (SPAN / most.astype(jnp.float32))[None] - OFFSET)
    code = jnp.where(groups < 0, -code, code)
    return code.reshape(sums.shape).astype(jnp.bfloat16), most


def decode(code, most):
    groups = code.astype(jnp.float32).reshape(-1, GROUP, code.shape[-1])
    size = (jnp.log2(jnp.abs(groups)) + OFFSET) * (most.astype(jnp.float32) * (1.0 / SPAN))[None]
    return jnp.where(groups < 0, -size, size).reshape(code.shape)


def kernel(
    tok, w, out, tbuf, mbuf, wbuf, code_out, code_in, acc,
    wl_sem, ws_sem, wr_sem, zs_sem, zr_sem, gs_sem, gr_sem, ms_sem, mr_sem, go_sem,
):
    z, q = lax.axis_index("row"), lax.axis_index("col")
    piece, half = tok.shape[0], tok.shape[1] // 2
    depth = w.shape[0]
    chunks = wbuf.shape[0]
    rows = tbuf.shape[1]
    blocks = code_out.shape[2]
    block = rows // blocks
    per = WIDTH // NARROW
    wide, narrow = chunks - FINE, FINE * per
    units = wide + narrow
    mine = z // 2
    own_slot = z % 2
    c, x, y = q % 2, (q // 2) % 2, q // 4
    over_x, over_y = q + 2 - 4 * x, q + 4 - 8 * y
    a = (1 - c) * over_x + c * over_y
    b = (1 - c) * over_y + c * over_x
    to_sib = 1 - 2 * c
    diagonal = over_x + over_y - q
    sib = q + to_sib
    barrier = pltpu.get_barrier_semaphore()

    def half_of(h):
        return tok.at[:, pl.ds(pl.multiple_of(h * half, half), half)]

    def block_of(k):
        return tok.at[:, pl.ds(pl.multiple_of(k * depth, depth), depth)]

    def place(kind, at):
        at = pl.ds(pl.multiple_of(at * piece, piece), piece)
        return mbuf.at[at, :] if kind == MO else tbuf.at[kind, at, :]

    def part(unit):
        if isinstance(unit, tuple):
            t = jnp.int32(unit[0])
            return wide + t, wide + lax.div(t, per), pl.ds(pl.multiple_of(lax.rem(t, per) * NARROW, NARROW), NARROW)
        return unit, unit, pl.ds(0, WIDTH)

    def columns(ref, unit):
        if isinstance(unit, tuple):
            t = jnp.int32(unit[0])
            return ref.at[:, pl.ds(pl.multiple_of(wide * WIDTH + t * NARROW, NARROW), NARROW)]
        return ref.at[:, pl.ds(pl.multiple_of(unit * WIDTH, WIDTH), WIDTH)]

    def each_unit(body):
        pl.loop(0, wide)(body)
        pl.loop(0, narrow)(lambda t: body((t,)))

    def remote(src, dst, send, recv, device):
        return pltpu.make_async_remote_copy(
            src_ref=src, dst_ref=dst, send_sem=send, recv_sem=recv, device_id=device, device_id_type=MESH
        )

    def start(copies):
        for copy in copies:
            copy.start()

    def greet(devices):
        for device in devices:
            pl.semaphore_signal(barrier, inc=1, device_id=device, device_id_type=MESH)
        pl.semaphore_wait(barrier, len(devices))

    def plane(kind, at, slot, device, src=None):
        here = place(kind, at)
        return remote(here if src is None else src, here, gs_sem.at[kind], gr_sem.at[kind, slot], (z, device))

    def own(kind, src=None):
        return [plane(kind, q, 0, a, src), plane(kind, q, 1, b, src), plane(kind, q, 3, sib, src)]

    def from_a(kind):
        return [plane(kind, a, 2, b), plane(kind, a, 3, sib)]

    def from_b(kind):
        return [plane(kind, b, 3, sib)]

    def from_d(kind):
        return [plane(kind, diagonal, 3, sib)]

    def pieces(kind, n):
        at = pl.ds(0, n * piece)
        return mbuf.at[at, :] if kind == MO else tbuf.at[kind, at, :]

    def sent(kind):
        remote(pieces(kind, 7), pieces(kind, 7), gs_sem.at[kind], gr_sem.at[kind, 0], (z, sib)).wait_send()

    def arrived(kind, n, slot, device):
        remote(pieces(kind, n), pieces(kind, n), gs_sem.at[kind], gr_sem.at[kind, slot], (z, device)).wait_recv()

    def on_a(kind):
        arrived(kind, 1, 0, a)
        start(from_a(kind))

    def on_b(kind):
        arrived(kind, 1, 1, b)
        start(from_b(kind))

    def on_d(kind):
        arrived(kind, 1, 2, b)
        start(from_d(kind))

    def finish(kind):
        arrived(kind, 4, 3, sib)

    def w_slot(unit, slot):
        _, j, lanes = part(unit)
        return wbuf.at[j, pl.ds(pl.multiple_of(slot * depth, depth), depth), lanes]

    def last_weight(n, slot, device):
        unit, deep = (narrow - 1,), depth // 2
        _, j, lanes = part(unit)
        at = pl.ds(pl.multiple_of(slot * depth + n * deep, deep), deep)
        src = columns(w.at[pl.ds(n * deep, deep), :], unit)
        return remote(src, wbuf.at[j, at, lanes], ws_sem.at[1 + n], wr_sem.at[units - 1 + n], device)

    def w_here(j):
        at = pl.ds(pl.multiple_of(own_slot * depth, depth), depth)
        return pltpu.make_async_copy(columns(w, j), wbuf.at[j, at, :], wl_sem.at[0])

    def rows_of(m):
        return pl.ds(m * block if isinstance(m, int) else pl.multiple_of(m * block, block), block)

    def sums(k, to, unit, m, device):
        u, j, lanes = part(unit)
        return remote(
            code_out.at[k, j, m, :, lanes], code_in.at[to, j, m, :, lanes], ms_sem.at[k], mr_sem.at[to, u, m], device
        )

    def product(kind, m, unit, slot=None):
        _, j, lanes = part(unit)
        if kind == MO:
            left, slot = mbuf[rows_of(m), :], own_slot
        elif slot is None:
            left = tbuf[kind, rows_of(m), :]
        else:
            left = tbuf[kind, rows_of(m), pl.ds(pl.multiple_of(slot * depth, depth), depth)]
        deep = slice(None) if slot is None else pl.ds(pl.multiple_of(slot * depth, depth), depth)
        return jnp.dot(left, wbuf[j, deep, lanes], preferred_element_type=jnp.float32)

    def ahead(kind, n):
        @pl.loop(0, blocks)
        def _(m):
            acc[kind, n, rows_of(m), :] = product(kind, m, wide + n, own_slot)

    def rest_of(kind, m, unit):
        _, j, lanes = part(unit)
        return acc[kind, j - wide, rows_of(m), lanes] + product(kind, m, unit, 1 - own_slot)

    def give(kind, k, to, unit, device):
        _, j, lanes = part(unit)

        @pl.loop(0, blocks)
        def _(m):
            if kind != MO and isinstance(unit, tuple):
                total = rest_of(kind, m, unit)
            else:
                total = product(kind, m, unit)
            code, most = encode(total)
            code_out[k, j, m, pl.ds(0, block), lanes] = code
            code_out[k, j, m, pl.ds(block, GROUP), lanes] = most
            sums(k, to, unit, m, device).start()

    def conclude(kind, senders, unit):
        _, j, lanes = part(unit)
        last = isinstance(unit, tuple)
        if last:
            @pl.loop(0, blocks)
            def _(m):
                acc[MS, j - wide, rows_of(m), lanes] = rest_of(kind, m, unit) if kind == MS else product(kind, m, unit)

        @pl.loop(0, blocks)
        def _(m):
            for to, device in enumerate(senders):
                sums(0, to, unit, m, device).wait_recv()
            total = acc[MS, j - wide, rows_of(m), lanes] if last else product(kind, m, unit)
            for to in range(len(senders)):
                total += decode(code_in[to, j, m, pl.ds(0, block), lanes], code_in[to, j, m, pl.ds(block, GROUP), lanes])
            at = wide * WIDTH + unit[0] * NARROW if last else unit * WIDTH
            wide_at = pl.ds(pl.multiple_of(jnp.int32(at), NARROW), NARROW if last else WIDTH)
            out[rows_of(m), wide_at] = total.astype(jnp.bfloat16)

    @pl.when((z == 0) | (z == LINE - 1))
    def outer():
        near, beyond = (1 + mine, q), (2 - mine, q)
        greet([near, beyond, (z, a), (z, b), (z, sib)])
        far_tokens = remote(half_of(1 - mine), place(TO, q), zs_sem.at[TO], zr_sem.at[TO], beyond)
        near_tokens = remote(block_of(1 + mine), place(MO, q), zs_sem.at[MO], zr_sem.at[MO], near)

        def weight(unit):
            return remote(columns(w, unit), w_slot(unit, own_slot), ws_sem.at[0], wr_sem.at[part(unit)[0]], near)

        near_tokens.start()
        weight(0).start()
        far_tokens.start()
        pl.loop(1, wide)(lambda j: weight(j).start())
        pl.loop(0, narrow - 2)(lambda t: weight((t,)).start())

        def last_units():
            weight((narrow - 2,)).start()
            for n in range(2):
                last_weight(n, own_slot, near).start()

        pl.when(c == 0)(last_units)
        start(own(MO, block_of(z)))
        mine_here = pltpu.make_async_copy(block_of(z), place(MO, q), zr_sem.at[MO])
        mine_here.start()
        pl.loop(0, chunks)(lambda j: w_here(j).start())
        on_a(MO)
        on_b(MO)
        on_d(MO)
        mine_here.wait()
        finish(MO)
        pltpu.make_async_copy(w, w, wl_sem.at[0]).wait()
        pl.loop(0, wide)(lambda j: conclude(MO, [near, beyond], j))
        far_tokens.wait_send()
        near_tokens.wait_send()
        sent(MO)

        @pl.when(c == 0)
        def _():
            last_weight(0, own_slot, near).wait_send()
            pl.semaphore_signal(go_sem, inc=1, device_id=(z, sib), device_id_type=MESH)

        @pl.when(c == 1)
        def _():
            pl.semaphore_wait(go_sem, 1)
            last_units()
            last_weight(0, own_slot, near).wait_send()

        last_weight(1, own_slot, near).wait_send()
        most = w.at[:, pl.ds(0, w.shape[1] - NARROW)]
        remote(most, most, ws_sem.at[0], wr_sem.at[0], near).wait_send()
        pl.loop(0, narrow)(lambda t: conclude(MO, [near, beyond], (t,)))

    @pl.when((z != 0) & (z != LINE - 1))
    def inner():
        end = mine * (LINE - 1)
        across, below, other_end = (LINE - 1 - z, q), (end, q), (LINE - 1 - end, q)
        greet([across, below, other_end, (z, a), (z, b), (z, sib)])
        own_half = half_of(mine)
        mine_here = pltpu.make_async_copy(own_half, place(MS, q), zr_sem.at[MS])

        def z_tokens(kind, device):
            src = block_of(z) if kind == MO else half_of(1 - mine)
            return remote(src, place(kind, q), zs_sem.at[kind], zr_sem.at[kind], device)

        def on_z(kind, device):
            z_tokens(kind, device).wait_recv()
            start(own(kind))

        def w_far(unit):
            u = part(unit)[0]
            return remote(columns(w, unit), w_slot(unit, 1 - own_slot), ws_sem.at[0], wr_sem.at[u], below)

        def to_across(unit):
            give(TS, 0, 0, unit, across)

        def to_other_end(unit):
            give(TO, 1, 1, unit, other_end)

        def to_below(unit):
            give(MO, 2, 0, unit, below)

        def finals(unit):
            conclude(MS, [across], unit)

        z_tokens(TS, across).start()
        mine_here.start()
        pl.loop(0, chunks)(lambda j: w_here(j).start())
        on_z(MO, below)
        on_z(TS, across)
        on_b(MO)
        on_a(TS)
        on_b(TS)
        on_d(TS)
        on_a(MO)
        finish(TS)
        pltpu.make_async_copy(w, w, wl_sem.at[0]).wait()
        w_far(0).wait_recv()
        to_across(0)
        on_d(MO)
        on_z(TO, other_end)
        finish(MO)
        pl.loop(0, wide)(to_below)
        on_a(TO)
        on_b(TO)
        w_far(1).wait_recv()
        to_across(1)
        on_d(TO)
        start(own(MS, own_half))
        finish(TO)
        pl.loop(0, 2)(to_other_end)
        pl.loop(0, narrow)(lambda t: to_below((t,)))
        w_far(2).wait_recv()
        to_other_end(2)
        to_across(2)
        mine_here.wait()
        on_a(MS)
        on_b(MS)
        on_d(MS)
        finish(MS)
        pl.loop(0, 2)(finals)

        @pl.loop(3, wide)
        def _(j):
            w_far(j).wait_recv()
            to_other_end(j)
            to_across(j)
            finals(j - 1)

            @pl.when(j == 3)
            def _():
                for kind in (TO, TS, MS):
                    pl.loop(0, FINE)(lambda n: ahead(kind, n))

        @pl.loop(0, narrow)
        def _(t):
            @pl.when(t < narrow - 1)
            def _():
                w_far((t,)).wait_recv()

            @pl.when(t == narrow - 1)
            def _():
                for n in range(2):
                    last_weight(n, 1 - own_slot, below).wait_recv()

            to_other_end((t,))
            to_across((t,))

            @pl.when(t == 1)
            def _():
                finals(wide - 1)

            @pl.when(t > 1)
            def _():
                finals((t - 2,))

        z_tokens(TS, across).wait_send()
        for kind in range(4):
            sent(kind)
        pl.loop(narrow - 2, narrow)(lambda t: finals((t,)))
        for k, device in enumerate((across, other_end, below)):
            remote(code_out.at[k], code_out.at[k], ms_sem.at[k], mr_sem.at[0, 0, 0], device).wait_send()


def line_plan(tokens, up_weight):
    piece, features = tokens.shape
    depth, columns = up_weight.shape
    rows, chunks, blocks = piece * PLANE, columns // WIDTH, 1
    units = chunks - FINE + FINE * WIDTH // NARROW
    dma, vmem, half = pltpu.SemaphoreType.DMA, pltpu.VMEM, jnp.bfloat16
    return pl.pallas_call(
        kernel,
        out_shape=pltpu.VMEM((rows, columns), jnp.bfloat16),
        in_specs=[pl.BlockSpec(memory_space=pl.ANY)] * 2,
        out_specs=pl.BlockSpec(memory_space=pltpu.VMEM),
        scratch_shapes=[
            vmem((3, rows, features // 2), half),
            vmem((rows, depth), half),
            vmem((chunks, 2 * depth, WIDTH), half),
            vmem((3, chunks, blocks, rows // blocks + GROUP, WIDTH), half),
            vmem((2, chunks, blocks, rows // blocks + GROUP, WIDTH), half),
            vmem((3, FINE, rows, WIDTH), jnp.float32),
            dma((1,)), dma((3,)), dma((units + 1,)),
            dma((4,)), dma((4,)),
            dma((4,)), dma((4, 4)),
            dma((3,)), dma((2, units, blocks)), pltpu.SemaphoreType.REGULAR,
        ],
        compiler_params=pltpu.CompilerParams(
            collective_id=0, has_side_effects=True, vmem_limit_bytes=62914560
        ),
        cost_estimate=pl.CostEstimate(
            flops=2 * rows * features * columns, bytes_accessed=2 * rows * features, transcendentals=0
        ),
    )(tokens, up_weight)


def solution(mesh):
    def on_device(tokens, up_weight):
        piece, features = tokens.shape
        depth, columns = up_weight.shape
        fits = columns >= (4 + FINE) * WIDTH and mesh.shape["row"] == LINE and mesh.shape["col"] == PLANE
        fits = fits and columns % WIDTH == 0 and piece % 16 == 0 and depth % 256 == 0 and features == LINE * depth
        return (line_plan if fits else gathered_weights)(tokens, up_weight)

    return jax.shard_map(
        on_device,
        mesh=mesh,
        in_specs=(P(("row", "col"), None), P("row", "col")),
        out_specs=P("row", "col"),
        check_vma=False,
    )
```
